32 devices in a mesh: node: 8 (over z, y), dev: 4 (over x, core).
Axes of the slice: x: 2, y: 2, z: 4, core: 2. Of those that a mesh axis runs over, the one named last changes fastest.
Arguments:
- tokens: bfloat16 [2048, 5120], P(('node', 'dev')), may hold values from -6 to 6
- node_ids: int32 [2048, 3], P(('node', 'dev')), may hold values from 0 to 7, all different within a row; in each aligned block of 64 rows (0 to 63, 64 to 127, ...) at most 25 rows name the same one
- expert_pick: int32 [2048, 6], P(('node', 'dev')), may hold values from 0 to 8, all different within a row
- gate_share: bfloat16 [2048, 6], P(('node', 'dev')), may hold values from 0.099609375 to 1
- gate_proj: bfloat16 [24, 1536, 5120], P('node', 'dev'), may hold values from -0.078125 to 0.078125
- up_proj: bfloat16 [24, 1536, 5120], P('node', 'dev'), may hold values from -0.078125 to 0.078125
- down_proj: bfloat16 [24, 1536, 5120], P('node', 'dev'), may hold values from -0.15625 to 0.15625
Outputs:
- moe_out: bfloat16 [2048, 5120], P(('node', 'dev'))
The draws below stay inside these ranges and needn't reach their ends.
Inputs may be any that keep to these rules, and one draw needn't show every extreme that they name: `node_ids`: A token names 3 different groups; at most 25 tokens of one device name one group, and some device reaches 25 in every draw. `expert_pick`: A token names 6 different picks; pick p selects local expert p % 3 of the token's group choice p // 3.
All inputs are finite; a program needn't handle non-finite values.
Results may differ from the reference program's by a relative error of at most 0.0085.
Values may be sent and summed in bfloat16 or wider, within the bound.
A program may use at most 256 MiB of HBM per device.

```python
import math
import jax
import jax.numpy as jnp
import numpy as np
from jax import lax

D = 5120
FF = 1536
TOP = 6
TOP_NODES = 3
EXP_NODE = 3
TOK_DEV = 64
EXPERTS = 24
CAP = 25
TOKENS = 2048
N_NODE = 8
N_DEV = 4


def level_of(rng, extent, pieces, least, largest):
    def one(axis_at, shards_of):
        steps = jax.random.uniform(jax.random.fold_in(jax.random.fold_in(rng, 6), axis_at), (shards_of,), jnp.float32, least / len(pieces), largest / len(pieces))
        return jnp.repeat(jnp.exp(steps), extent[axis_at] // shards_of).reshape((-1,) + (1,) * (len(extent) - axis_at - 1))

    gain = one(*pieces[0])
    for cut in pieces[1:]:
        gain = gain * one(*cut)
    return gain


def different_ones(own_key, rows, count, top, lift):
    order = jax.random.permutation(jax.random.fold_in(own_key, 1), count)
    pull = order
    for power in range(3):
        pull = pull * pull // count
    pull = pull * lift // count
    lots = jax.random.randint(jax.random.fold_in(own_key, 2), (rows, count), 0, 4096) + pull
    fixed_rows = jax.random.permutation(jax.random.fold_in(own_key, 3), rows)[jnp.arange(count) % rows]
    lots = jnp.where(jnp.arange(rows)[:, None] == fixed_rows[None, :], 1 << 14, lots)
    merit = lots * count + jnp.arange(count)
    return lax.top_k(merit.astype(jnp.int32), top)[1].astype(jnp.int32)


def deal_out(rng, own, number, rows, count, top, bound, lean):
    sequence = jax.random.permutation(rng, count)
    packed, common = portions_of(count, rows * top, bound, lean, True), portions_of(count, rows * top, bound, lean, False)
    places = jnp.arange(count)

    def named(lengths, offset_by):
        used = int((lengths > 0).sum())
        fixed = max(1, used // 4)
        passed = fixed + (places - fixed + offset_by * (used - fixed)) % max(1, count - fixed)
        return jnp.zeros((count,), jnp.int32).at[sequence[jnp.where(places < fixed, places, passed)]].set(jnp.asarray(lengths, jnp.int32))

    lengths = jnp.where(number % 4 == 0, named(packed, number // 4), named(common, number - number // 4 - 1))
    mixed = jax.random.permutation(jax.random.fold_in(own, 3), count)
    donor, receiver = mixed[0:count // 2 * 2:2], mixed[1:count // 2 * 2:2]
    slack = jnp.minimum(lengths[donor] - 1, bound - lengths[receiver]) // 2
    slack = jnp.where((donor == sequence[0]) | (receiver == sequence[0]) | (lengths[receiver] == 0), 0, jnp.maximum(slack, 0))
    passed = jax.random.randint(jax.random.fold_in(own, 4), (count // 2,), 0, 1 << 20) % (slack + 1)
    lengths = lengths.at[donor].add(-passed).at[receiver].add(passed)
    members = jnp.searchsorted(jnp.cumsum(lengths), jnp.arange(rows * top), side="right").astype(jnp.int32)
    table = members.reshape(top, rows).T
    table = table[jax.random.permutation(jax.random.fold_in(own, 1), rows)]
    offset_by = jax.random.randint(jax.random.fold_in(own, 2), (rows, 1), 0, top)
    return jnp.take_along_axis(table, (jnp.arange(top)[None, :] + offset_by) % top, axis=1)


def portions_of(count, total, bound, slope, full):
    loads = [(1 << 20) // math.isqrt(grade ** slope) + 1 for grade in range(1, count + 1)]
    largest = bound if full else min(bound, max(-(-total // count), total * loads[0] // sum(loads)))
    least = 1 if total - largest >= count - 1 else 0
    given, surplus = [largest] + [least] * (count - 1), total - largest - least * (count - 1)
    while surplus > 0:
        free = [i for i in range(1, count) if given[i] < largest] or [i for i in range(1, count) if given[i] < bound]
        whole, left = sum([loads[i] for i in free]), surplus
        for i in free:
            extra = min(bound - given[i], max(1, left * loads[i] // whole), surplus)
            given[i] = given[i] + extra
            surplus = surplus - extra
    return np.array(given)


def noise(key, dims, spread, bound, cuts=(), kind=jnp.bfloat16):
    drawn = jax.random.normal(key, dims, jnp.float32) * spread
    if len(cuts) > 0:
        drawn = level_of(key, dims, cuts, -0.22, 0.18) * drawn
    return jnp.clip(drawn, min=-bound, max=bound).astype(kind)


def setup_inputs(seed: int = 0) -> dict:
    streams_of = jax.random.split(jax.random.key(seed), 8)
    tokens = noise(streams_of[0], (TOKENS, D), 1.0, 6.0, ((0, 32),))
    node_ids_keys = jax.random.split(jax.random.fold_in(streams_of[1], 1), TOKENS // TOK_DEV)
    node_ids_turns = jax.random.permutation(jax.random.fold_in(streams_of[1], 3), TOKENS // TOK_DEV)
    node_ids = jax.vmap(lambda own, number: deal_out(jax.random.fold_in(streams_of[1], 2), own, number, TOK_DEV, N_NODE, TOP_NODES, CAP, 2))(node_ids_keys, node_ids_turns).reshape((TOKENS, TOP_NODES))
    expert_pick = different_ones(streams_of[2], TOKENS, TOP_NODES * EXP_NODE, TOP, 0)
    gate_share = jnp.clip(jnp.exp(math.log(1.0) - 2.306499 * jax.random.uniform(streams_of[3], (TOKENS, TOP), jnp.float32) ** level_of(streams_of[3], (TOKENS, TOP), ((0, 32),), -0.2, 0.2)), 0.099609375, 1.0).astype(jnp.bfloat16)
    gate_proj = noise(streams_of[4], (EXPERTS, FF, D), D ** -0.5, 0.078125, ((0, 8), (1, 4)))
    up_proj = noise(streams_of[5], (EXPERTS, FF, D), D ** -0.5, 0.078125, ((0, 8), (1, 4)))
    down_proj = noise(streams_of[6], (EXPERTS, FF, D), FF ** -0.5, 0.15625, ((0, 8), (1, 4)))
    return {"tokens": tokens, "node_ids": node_ids, "expert_pick": expert_pick, "gate_share": gate_share, "gate_proj": gate_proj, "up_proj": up_proj, "down_proj": down_proj}


def reference(tokens, node_ids, expert_pick, gate_share, gate_proj, up_proj, down_proj):
    token_count = tokens.shape[0]
    capacity = CAP * N_NODE * N_DEV
    candidates = TOP_NODES * EXP_NODE
    slice_width = FF // N_DEV
    picked = (expert_pick[:, :, None] == jnp.arange(candidates, dtype=jnp.int32)[None, None, :]).astype(jnp.float32)
    shares = jnp.einsum('tj,tjq->tq', gate_share.astype(jnp.float32), picked, precision=lax.Precision.HIGHEST)
    shares = shares.reshape(token_count, TOP_NODES, EXP_NODE)
    contract = (((1,), (1,)), ((), ()))

    def per_node(total, node_index):
        hit_mask = (node_ids == node_index).astype(jnp.int32)
        chosen = jnp.sum(hit_mask, axis=1) > 0
        positions = jnp.nonzero(chosen, size=capacity, fill_value=0)[0].astype(jnp.int32)
        is_valid = (jnp.arange(capacity, dtype=jnp.int32) < jnp.sum(chosen.astype(jnp.int32))).astype(jnp.float32)
        node_shares = jnp.einsum('tk,tke->te', hit_mask.astype(jnp.float32), shares, precision=lax.Precision.HIGHEST)
        node_shares = node_shares[positions] * is_valid[:, None]
        tok_rows = tokens[positions]
        accumulated = jnp.zeros((capacity, N_DEV, D), jnp.float32)
        for expert_local in range(EXP_NODE):
            expert = (node_index * EXP_NODE + expert_local).astype(jnp.int32)
            w_gate = lax.dynamic_index_in_dim(gate_proj, expert, 0, keepdims=False)
            w_up = lax.dynamic_index_in_dim(up_proj, expert, 0, keepdims=False)
            w_down = lax.dynamic_index_in_dim(down_proj, expert, 0, keepdims=False)
            gate_val = lax.dot_general(tok_rows, w_gate, contract, preferred_element_type=jnp.float32)
            up_val = lax.dot_general(tok_rows, w_up, contract, preferred_element_type=jnp.float32)
            hidden = (jax.nn.silu(gate_val) * up_val).astype(jnp.bfloat16)
            grouped = jnp.einsum('rgf,gfd->rgd', hidden.reshape(capacity, N_DEV, slice_width).astype(jnp.float32),
                                 w_down.reshape(N_DEV, slice_width, D).astype(jnp.float32),
                                 precision=lax.Precision.HIGHEST)
            accumulated = accumulated + node_shares[:, expert_local, None, None] * grouped
        partial_value = lax.optimization_barrier(accumulated.astype(jnp.bfloat16)).astype(jnp.float32)
        contrib = jnp.sum(partial_value, axis=1) * is_valid[:, None]
        return total.at[positions].add(contrib), None

    total, _ = lax.scan(per_node, jnp.zeros((token_count, D), jnp.float32), jnp.arange(N_NODE, dtype=jnp.int32))
    return total.astype(jnp.bfloat16)
```

```python
import jax
import jax.numpy as jnp
from jax import lax
from jax.sharding import PartitionSpec as P


LANES = 128
TILE = 8
CHUNKS = 2
F32 = jnp.float32
BF16 = jnp.bfloat16


def swap(value, axis, mask):
    count = lax.axis_size(axis)
    return lax.ppermute(value, axis, [(i, i ^ mask) for i in range(count)])


def round_up(value, unit):
    return -(-value // unit) * unit


def shards(tokens, node_ids, expert_pick, gate_share, gate_proj, up_proj, down_proj):
    tok_count, width = tokens.shape
    nodes = lax.axis_size("node")
    devs = lax.axis_size("dev")
    me = lax.axis_index("node")
    dev = lax.axis_index("dev")
    choices = node_ids.shape[1]
    local = gate_proj.shape[0]
    hidden_width = gate_proj.shape[1]
    part = width // devs
    capacity = devs * (choices * tok_count // nodes + 1)
    slots = round_up(capacity + 1, TILE)
    pool = devs * tok_count

    order = me ^ jnp.arange(nodes, dtype=jnp.int32)
    picked = (
        expert_pick[:, :, None] == jnp.arange(choices * local, dtype=jnp.int32)[None, None, :]
    )
    shares = jnp.sum(jnp.where(picked, gate_share[:, :, None].astype(F32), 0.0), axis=1)
    shares = shares.reshape(tok_count, choices, local)
    chosen = node_ids[:, :, None] == order[None, None, :]
    gates = jnp.sum(
        jnp.where(chosen[:, :, :, None], shares[:, :, None, :], 0.0), axis=1
    )
    gates = gates.transpose(0, 2, 1).reshape(tok_count, local * nodes).astype(BF16)
    gates = jnp.pad(gates, ((0, 0), (0, LANES - local * nodes)))

    def cut(array, q, axis):
        return lax.dynamic_slice_in_dim(array, (dev ^ q) * part, part, axis)

    pieces = []
    for q in range(devs):
        piece = jnp.concatenate([cut(tokens, q, 1), gates], axis=1)
        pieces.append(swap(piece, "dev", q) if q else piece)
    pooled = jnp.concatenate(pieces, axis=0)
    place = (dev ^ jnp.arange(devs, dtype=jnp.int32))[:, None] * tok_count + jnp.arange(
        tok_count, dtype=jnp.int32
    )
    place = place.reshape(pool)
    feats = pooled[:, :part]
    pool_gates = pooled[:, part : part + local * nodes].reshape(pool, local, nodes)
    mask = (jnp.max(pool_gates, axis=1) > 0).astype(BF16)
    earlier = (place[None, :] < place[:, None]).astype(BF16)
    before = jnp.dot(earlier, mask, preferred_element_type=F32).astype(jnp.int32)
    slot_of = jnp.where(mask > 0, before, -1)
    select = (
        slot_of.T[:, None, :] == jnp.arange(slots, dtype=jnp.int32)[None, :, None]
    ).astype(BF16)
    send = jnp.dot(
        select.reshape(nodes * slots, pool), feats, preferred_element_type=F32
    ).astype(BF16)
    send = send.reshape(nodes, slots, part)
    gate_rows = jnp.einsum(
        "tek,kct->kec", pool_gates, select, preferred_element_type=F32
    ).astype(BF16)
    gate_rows = jnp.pad(gate_rows, ((0, 0), (0, 0), (0, LANES - slots)))
    gate_rows = gate_rows.reshape(nodes, 1, local * LANES)
    gate_rows = jnp.pad(gate_rows, ((0, 0), (0, 0), (0, part - local * LANES)))
    last = jnp.arange(slots, dtype=jnp.int32)[None, :, None] == slots - 1
    send = jnp.where(last, gate_rows, send)

    w_gate = gate_proj.reshape(local * hidden_width, width)
    w_up = up_proj.reshape(local * hidden_width, width)
    w_down = down_proj.reshape(local * hidden_width, width)

    tiles = slots // TILE
    bounds = [tiles * i // CHUNKS * TILE for i in range(CHUNKS + 1)]
    spans = list(zip(bounds[:-1], bounds[1:]))[::-1]

    got = []
    for low, high in spans:
        blocks = [send[0, low:high]]
        for k in range(1, nodes):
            blocks.append(swap(send[k, low:high], "node", k))
        got.append(jnp.concatenate(blocks, axis=0))

    g = got[0].reshape(nodes, -1, part)[:, -1, : local * LANES]
    g = g.reshape(nodes, local, LANES)[:, :, :slots]

    contract = (((1,), (1,)), ((), ()))
    far_first = [1 << i for i in range(devs.bit_length() - 1)][::-1]
    gated = []
    for (low, high), rows in zip(spans, got):
        count = nodes * (high - low)
        sources = {0: rows}
        for bit in far_first:
            for q in list(sources):
                sources[q ^ bit] = swap(sources[q], "dev", bit)
        gate_val = up_val = 0.0
        for q, source in sorted(sources.items()):
            gate_val += lax.dot_general(source, cut(w_gate, q, 1), contract, preferred_element_type=F32)
            up_val += lax.dot_general(source, cut(w_up, q, 1), contract, preferred_element_type=F32)
        scale = g[:, :, low:high].transpose(0, 2, 1).reshape(count, local).astype(F32)
        act = (jax.nn.silu(gate_val) * up_val).reshape(count, local, hidden_width)
        act = (act * scale[:, :, None]).astype(BF16).reshape(count, local * hidden_width)
        gated.append(act)

    total = 0.0
    for (low, high), act in zip(spans, gated):
        span = high - low

        def product(q):
            return jnp.dot(act, cut(w_down, q, 1), preferred_element_type=F32)

        sums = {q: product(q) for q in range(devs)[::-1]}
        for bit in far_first[::-1]:
            for q in [q for q in sums if q & bit]:
                sums[q ^ bit] += swap(sums.pop(q).astype(BF16), "dev", bit).astype(F32)
        summed = sums[0].astype(BF16).reshape(nodes, span, part)
        blocks = [summed[0]]
        for k in range(1, nodes):
            blocks.append(swap(summed[k], "node", k))
        back = jnp.concatenate(blocks, axis=0)
        spread = select[:, low:high].reshape(nodes * span, pool)
        total += lax.dot_general(
            spread, back, (((0,), (0,)), ((), ())), preferred_element_type=F32
        )

    total = total.astype(BF16).reshape(devs, tok_count, part)
    output = jnp.zeros((tok_count, width), BF16)
    for q in range(devs):
        piece = swap(total[q], "dev", q) if q else total[0]
        output = lax.dynamic_update_slice_in_dim(output, piece, (dev ^ q) * part, 1)
    return output


def solution(mesh):
    return jax.shard_map(
        shards,
        mesh=mesh,
        in_specs=(
            P(("node", "dev"), None),
            P(("node", "dev"), None),
            P(("node", "dev"), None),
            P(("node", "dev"), None),
            P("node", "dev", None),
            P("node", "dev", None),
            P("node", "dev", None),
        ),
        out_specs=P(("node", "dev"), None),
        check_vma=False,
    )
```
